32 devices in a mesh: dp: 2 (over x), expert: 16 (over z, y, core).
Axes of the slice: x: 2, y: 2, z: 4, core: 2. Of those that a mesh axis runs over, the one named last changes fastest.
Arguments:
- tokens: bfloat16 [512, 2048], P('expert', 'dp'), may hold values from -6 to 6
- routes: int32 [512, 8], P('expert'), may hold values from 0 to 63, all different within a row; in each aligned block of 32 rows (0 to 31, 32 to 63, ...) at most 4 rows name the same one
- route_weight: float32 [512, 8], P('expert'), may hold values from 0.05 to 0.5
- gate_weight: bfloat16 [64, 2048, 768], P('expert', 'dp'), may hold values from -0.125 to 0.125
- up_weight: bfloat16 [64, 2048, 768], P('expert', 'dp'), may hold values from -0.125 to 0.125
- down_weight: bfloat16 [64, 768, 2048], P('expert', None, 'dp'), may hold values from -0.21875 to 0.21875
- trained_down: float32 [64, 768, 2048], P('expert', 'dp'), may hold values from -0.21875 to 0.21875
Outputs:
- mixed: bfloat16 [512, 2048], P('expert', 'dp')
- synced_down: bfloat16 [64, 768, 2048], P('expert', None, 'dp')
The draws below stay inside these ranges and needn't reach their ends.
Inputs may be any that keep to these rules, and one draw needn't show every extreme that they name: `routes`: each row names 8 different experts. Among the 32 rows of one device (aligned blocks), no expert is named more than 4 times, a bound that some block reaches.
All inputs are finite; a program needn't handle non-finite values.
Results may differ from the reference program's by a relative error of at most 0.0058.
Values may be sent and summed in bfloat16 or wider, within the bound.
No kernel may reach another device: no remote copies, remote signals or barrier semaphores. Data moves between devices by JAX's collectives and lax.ppermute only.
A program may use at most 128 MiB of HBM per device.

```python
import math
import jax
import jax.numpy as jnp
import numpy as np
from jax import lax

D = 2048
FF = 768
TOP = 8
EXPERTS = 64
TOK_DEV = 32
CAP = 4
TOKENS = 512


def level_of(stream_key, extent, pieces, least, high):
    loudness = 1.0
    for dim, parts in pieces:
        heights = jax.random.uniform(jax.random.fold_in(jax.random.fold_in(stream_key, 6), dim), (parts,), jnp.float32, least / len(pieces), high / len(pieces))
        loudness = loudness * jnp.repeat(jnp.exp(heights), extent[dim] // parts).reshape((-1,) + (1,) * (len(extent) - 1 - dim))
    return loudness


def routed_block(key, own, number, rows, amount, top, limit, lean):
    order = jax.random.permutation(key, amount)
    crowded, common = shares(amount, rows * top, limit, lean, True), shares(amount, rows * top, limit, lean, False)
    places = jnp.arange(amount)

    def named(lengths, turn):
        used = int((lengths > 0).sum())
        fixed = max(1, used // 4)
        shifted = fixed + (places - fixed + turn * (used - fixed)) % max(1, amount - fixed)
        return jnp.zeros((amount,), jnp.int32).at[order[jnp.where(places < fixed, places, shifted)]].set(jnp.asarray(lengths, jnp.int32))

    lengths = jnp.where(number % 4 == 0, named(crowded, number // 4), named(common, number - number // 4 - 1))
    mixed = jax.random.permutation(jax.random.fold_in(own, 3), amount)
    giver, receiver = mixed[0:amount // 2 * 2:2], mixed[1:amount // 2 * 2:2]
    margin = jnp.minimum(lengths[giver] - 1, limit - lengths[receiver]) // 2
    margin = jnp.where((giver == order[0]) | (receiver == order[0]) | (lengths[receiver] == 0), 0, jnp.maximum(margin, 0))
    shifted = jax.random.randint(jax.random.fold_in(own, 4), (amount // 2,), 0, 1 << 20) % (margin + 1)
    lengths = lengths.at[giver].add(-shifted).at[receiver].add(shifted)
    items = jnp.searchsorted(jnp.cumsum(lengths), jnp.arange(rows * top), side="right").astype(jnp.int32)
    grid = items.reshape(top, rows).T
    grid = grid[jax.random.permutation(jax.random.fold_in(own, 1), rows)]
    turn = jax.random.randint(jax.random.fold_in(own, 2), (rows, 1), 0, top)
    return jnp.take_along_axis(grid, (jnp.arange(top)[None, :] + turn) % top, axis=1)


def shares(number_of, total, most, slope, full):
    loads = [(1 << 20) // math.isqrt(standing ** slope) + 1 for standing in range(1, number_of + 1)]
    largest = most if full else min(most, max(-(-total // number_of), total * loads[0] // sum(loads)))
    least = 1 if total - largest >= number_of - 1 else 0
    given, spare = [largest] + [least] * (number_of - 1), total - largest - least * (number_of - 1)
    while spare > 0:
        movable = [i for i in range(1, number_of) if given[i] < largest] or [i for i in range(1, number_of) if given[i] < most]
        pool, remaining = sum([loads[i] for i in movable]), spare
        for i in movable:
            addition = min(most - given[i], max(1, remaining * loads[i] // pool), spare)
            given[i] = given[i] + addition
            spare = spare - addition
    return np.array(given)


def noise(key, extent, width, reach, split=(), kind=jnp.bfloat16):
    loudness = level_of(key, extent, split, -0.22, 0.18) if split else 1.0
    drawn = jax.random.normal(key, extent, jnp.float32) * width * loudness
    return jnp.minimum(jnp.maximum(drawn, -reach), reach).astype(kind)


def setup_inputs(seed: int = 0) -> dict:
    key_list = jax.random.split(jax.random.key(seed), 8)
    tokens = noise(key_list[0], (TOKENS, D), 1.0, 6.0, ((0, 16), (1, 2)))
    routes_keys = jax.random.split(jax.random.fold_in(key_list[1], 1), TOKENS // TOK_DEV)
    routes_turns = jax.random.permutation(jax.random.fold_in(key_list[1], 3), TOKENS // TOK_DEV)
    routes = jax.vmap(lambda own, number: routed_block(jax.random.fold_in(key_list[1], 2), own, number, TOK_DEV, EXPERTS, TOP, CAP, 2))(routes_keys, routes_turns).reshape((TOKENS, TOP))
    route_weight = jnp.clip(jnp.exp(math.log(0.5) - 2.3025851 * jax.random.uniform(key_list[2], (TOKENS, TOP), jnp.float32) ** level_of(key_list[2], (TOKENS, TOP), ((0, 16),), -0.2, 0.2)), 0.05, 0.5)
    gate_weight = noise(key_list[3], (EXPERTS, D, FF), D ** -0.5, 0.125, ((0, 16), (1, 2)))
    up_weight = noise(key_list[4], (EXPERTS, D, FF), D ** -0.5, 0.125, ((0, 16), (1, 2)))
    down_weight = noise(key_list[5], (EXPERTS, FF, D), FF ** -0.5, 0.21875, ((0, 16), (2, 2)))
    trained_down = noise(key_list[6], (EXPERTS, FF, D), FF ** -0.5, 0.21875, ((0, 16), (1, 2)), jnp.float32)
    return {"tokens": tokens, "routes": routes, "route_weight": route_weight, "gate_weight": gate_weight, "up_weight": up_weight, "down_weight": down_weight, "trained_down": trained_down}


def reference(tokens, routes, route_weight, gate_weight, up_weight, down_weight, trained_down):
    blocks = TOKENS // TOK_DEV
    labels = jnp.arange(EXPERTS, dtype=jnp.int32)
    counts = jnp.sum((routes[:, :, None] == labels[None, None, :]).astype(jnp.int32), axis=1)
    per_block = counts.reshape(blocks, TOK_DEV, EXPERTS)
    earlier = (jnp.cumsum(per_block, axis=1) - per_block).reshape(TOKENS, EXPERTS).astype(jnp.int32)
    slot_index = jnp.take_along_axis(earlier, routes, axis=1).astype(jnp.int32)
    block_of = (jnp.arange(TOKENS, dtype=jnp.int32) // TOK_DEV)[:, None]
    position = (block_of * CAP + slot_index).astype(jnp.int32)
    rows_expert = blocks * CAP
    token_ids = jnp.broadcast_to(jnp.arange(TOKENS, dtype=jnp.int32)[:, None], routes.shape)
    row_table = jnp.full((EXPERTS, rows_expert), TOKENS, jnp.int32).at[routes, position].set(token_ids)
    padded = jnp.concatenate([tokens, jnp.zeros((1, D), tokens.dtype)], axis=0)

    def one_expert(operands):
        row_index, gate_mat, up_mat, down_mat = operands
        gathered = padded[row_index]
        gate_pre = jnp.dot(gathered, gate_mat, preferred_element_type=jnp.float32)
        up_pre = jnp.dot(gathered, up_mat, preferred_element_type=jnp.float32)
        hidden = (jax.nn.silu(gate_pre) * up_pre).astype(jnp.bfloat16)
        return jnp.dot(hidden, down_mat, preferred_element_type=jnp.float32).astype(jnp.bfloat16)

    results = lax.map(one_expert, (row_table, gate_weight, up_weight, down_weight))
    picked = results[routes, position]
    mixed = jnp.sum(route_weight[:, :, None] * picked.astype(jnp.float32), axis=1).astype(jnp.bfloat16)
    return mixed, trained_down.astype(jnp.bfloat16)
```

```python
import jax
import jax.numpy as jnp
from jax import lax
from jax.sharding import PartitionSpec as P


CAP = 4
PIECES = 2


def ring(size, shift):
    return [(i, (i + shift) % size) for i in range(size)]


def local(tokens, routes, route_weight, gate_weight, up_weight, down_weight, trained_down):
    tok_rows, width_local = tokens.shape
    expert_local, hid, _ = down_weight.shape
    trained_rows = trained_down.shape[1]
    groups = lax.axis_size("expert")
    ways = lax.axis_size("dp")
    me = lax.axis_index("dp")
    experts_all = expert_local * groups
    capacity = CAP
    rows = groups * capacity
    share = rows // ways
    piece = trained_rows // PIECES

    def columns(source, expert, part, owner):
        strip = source[expert, part * piece:(part + 1) * piece]
        if ways == 2:
            strip = jnp.where(owner == 0, strip[:, :width_local], strip[:, width_local:])
        else:
            strip = lax.dynamic_slice_in_dim(strip, owner * width_local, width_local, 1)
        return strip.astype(jnp.bfloat16)

    arrivals = {}
    order = [(e, p) for e in range(expert_local) for p in range(PIECES)]
    for expert, part in order:
        arrivals[expert, part] = [
            lax.ppermute(columns(trained_down, expert, part, (me + s) % ways), "dp", ring(ways, s))
            for s in range(1, ways)
        ]

    labels = lax.broadcasted_iota(jnp.int32, (1, 1, experts_all), 2)
    chosen = routes[:, :, None] == labels
    counts = jnp.sum(chosen.astype(jnp.int32), axis=1)
    earlier = jnp.cumsum(counts, axis=0) - counts
    weight_expert = jnp.sum(jnp.where(chosen, route_weight[:, :, None], 0.0), axis=1)
    slot_ids = lax.broadcasted_iota(jnp.int32, (1, 1, capacity), 2)
    placed = (counts[:, :, None] == 1) & (earlier[:, :, None] == slot_ids)
    dispatch = placed.astype(jnp.bfloat16).reshape(tok_rows, experts_all * capacity)
    outgoing = jnp.dot(dispatch.T, tokens, preferred_element_type=jnp.float32).astype(jnp.bfloat16)
    own_source, outgoing = lax.optimization_barrier((trained_down, outgoing))
    outgoing = outgoing.reshape(groups, expert_local, capacity, width_local)
    arrived = lax.all_to_all(outgoing, "expert", split_axis=0, concat_axis=2, tiled=True)
    arrived = arrived.reshape(expert_local, rows, width_local)

    gate_part = jnp.einsum("erd,edf->erf", arrived, gate_weight, preferred_element_type=jnp.float32)
    up_part = jnp.einsum("erd,edf->erf", arrived, up_weight, preferred_element_type=jnp.float32)
    gate_part = gate_part.reshape(expert_local, ways, share, hid)
    up_part = up_part.reshape(expert_local, ways, share, hid)

    def share_of(array, owner):
        return lax.dynamic_index_in_dim(array, owner, 1, keepdims=False)

    gate_sum = share_of(gate_part, me)
    up_sum = share_of(up_part, me)
    for s in range(1, ways):
        owner = (me + s) % ways
        pair = jnp.stack([share_of(gate_part, owner), share_of(up_part, owner)]).astype(jnp.bfloat16)
        pair = lax.ppermute(pair, "dp", ring(ways, s))
        gate_sum = gate_sum + pair[0].astype(jnp.float32)
        up_sum = up_sum + pair[1].astype(jnp.float32)
    hidden_own = (jax.nn.silu(gate_sum) * up_sum).astype(jnp.bfloat16)
    hidden = jnp.zeros((expert_local, ways, share, hid), jnp.bfloat16)
    hidden = lax.dynamic_update_index_in_dim(hidden, hidden_own, me, 1)
    for s in range(1, ways):
        other = lax.ppermute(hidden_own, "dp", ring(ways, s))
        hidden = lax.dynamic_update_index_in_dim(hidden, other, (me - s) % ways, 1)
    hidden = hidden.reshape(expert_local, rows, hid)

    expert_out = jnp.einsum("erf,efd->erd", hidden, down_weight, preferred_element_type=jnp.float32)
    expert_out = expert_out.astype(jnp.bfloat16).reshape(1, expert_local, rows, width_local)
    returned = lax.all_to_all(expert_out, "expert", split_axis=2, concat_axis=0, tiled=True)
    returned = returned.reshape(experts_all * capacity, width_local)
    combine = (weight_expert[:, :, None] * placed.astype(jnp.float32)).reshape(
        tok_rows, experts_all * capacity
    )
    mixed = jnp.dot(
        combine,
        returned.astype(jnp.float32),
        precision=lax.Precision.HIGHEST,
        preferred_element_type=jnp.float32,
    )
    mixed = mixed.astype(jnp.bfloat16)

    synced = jnp.zeros((expert_local, ways, trained_rows, width_local), jnp.bfloat16)
    for expert, part in order:
        own = columns(own_source, expert, part, me)
        synced = lax.dynamic_update_slice(synced, own[None, None], (expert, me, part * piece, 0))
    for expert, part in order:
        for s in range(1, ways):
            arrival = arrivals[expert, part][s - 1]
            synced = lax.dynamic_update_slice(synced, arrival[None, None], (expert, (me - s) % ways, part * piece, 0))
    synced_down = synced.reshape(expert_local, ways * trained_rows, width_local)
    return (mixed, synced_down)


def solution(mesh):
    placed = (
        P("expert", "dp"),
        P("expert", None),
        P("expert", None),
        P("expert", "dp", None),
        P("expert", "dp", None),
        P("expert", None, "dp"),
        P("expert", "dp", None),
    )

    return jax.shard_map(
        local,
        mesh=mesh,
        in_specs=placed,
        out_specs=(P("expert", "dp"), P("expert", None, "dp")),
        check_vma=False,
    )
```

```python
import jax
import jax.numpy as jnp
from jax import lax
from jax.experimental import pallas as pl
from jax.experimental.pallas import tpu as pltpu
from jax.sharding import PartitionSpec as P


CAP = 4
PIECES = 2


def ring(size, shift):
    return [(i, (i + shift) % size) for i in range(size)]


def narrow(where, trained, synced, expert, part, piece, ways, width):
    experts, trained_rows, _ = trained.shape
    step = 64 if piece % 64 == 0 else piece
    steps = piece // step

    def body(where_ref, strip_ref, *refs):
        sent_ref, own_ref = refs[-2:]
        for s in range(ways):
            owner = lax.rem(where_ref[0] + s, ways)
            columns = strip_ref[0, :, pl.ds(pl.multiple_of(owner * width, 128), width)]
            if s:
                sent_ref[s - 1] = columns.astype(jnp.bfloat16)
            else:
                own_ref[0, 0] = columns.astype(jnp.bfloat16)

    in_specs = [pl.BlockSpec((1, step, ways * width), lambda i, w: (expert, part * steps + i, 0))]
    operands = [where, trained]
    if synced is not None:
        in_specs.append(pl.BlockSpec(memory_space=pl.ANY))
        operands.append(synced)
    return pl.pallas_call(
        body,
        grid_spec=pltpu.PrefetchScalarGridSpec(
            num_scalar_prefetch=1,
            grid=(steps,),
            in_specs=in_specs,
            out_specs=[
                pl.BlockSpec((ways - 1, step, width), lambda i, w: (0, i, 0)),
                pl.BlockSpec((1, 1, step, width), lambda i, w: (expert, w[0], part * steps + i, 0)),
            ],
        ),
        out_shape=[
            jax.ShapeDtypeStruct((ways - 1, piece, width), jnp.bfloat16),
            jax.ShapeDtypeStruct((experts, ways, trained_rows, width), jnp.bfloat16),
        ],
        input_output_aliases={} if synced is None else {2: 1},
    )(*operands)


def local(tokens, routes, route_weight, gate_weight, up_weight, down_weight, trained_down):
    tok_rows, width_local = tokens.shape
    expert_local, hid, _ = down_weight.shape
    trained_rows = trained_down.shape[1]
    groups = lax.axis_size("expert")
    ways = lax.axis_size("dp")
    me = lax.axis_index("dp")
    experts_all = expert_local * groups
    capacity = CAP
    rows = groups * capacity
    share = rows // ways
    pieces = PIECES if trained_rows % (16 * PIECES) == 0 else 1
    piece = trained_rows // pieces
    where = me.astype(jnp.int32).reshape(1)

    arrivals = {}
    synced = None
    order = [(e, p) for e in range(expert_local) for p in range(pieces)]
    for expert, part in order:
        sent, synced = narrow(where, trained_down, synced, expert, part, piece, ways, width_local)
        arrivals[expert, part] = [
            lax.ppermute(sent[s - 1], "dp", ring(ways, s)) for s in range(1, ways)
        ]

    labels = lax.broadcasted_iota(jnp.int32, (1, 1, experts_all), 2)
    chosen = routes[:, :, None] == labels
    counts = jnp.sum(chosen.astype(jnp.int32), axis=1)
    earlier = jnp.cumsum(counts, axis=0) - counts
    weight_expert = jnp.sum(jnp.where(chosen, route_weight[:, :, None], 0.0), axis=1)
    slot_ids = lax.broadcasted_iota(jnp.int32, (1, 1, capacity), 2)
    placed = (counts[:, :, None] == 1) & (earlier[:, :, None] == slot_ids)
    dispatch = placed.astype(jnp.bfloat16).reshape(tok_rows, experts_all * capacity)
    outgoing = jnp.dot(dispatch.T, tokens, preferred_element_type=jnp.float32).astype(jnp.bfloat16)
    outgoing = outgoing.reshape(groups, expert_local, capacity, width_local)
    arrived = lax.all_to_all(outgoing, "expert", split_axis=0, concat_axis=2, tiled=True)
    arrived = arrived.reshape(expert_local, rows, width_local)

    gate_part = jnp.einsum("erd,edf->erf", arrived, gate_weight, preferred_element_type=jnp.float32)
    up_part = jnp.einsum("erd,edf->erf", arrived, up_weight, preferred_element_type=jnp.float32)
    gate_part = gate_part.reshape(expert_local, ways, share, hid)
    up_part = up_part.reshape(expert_local, ways, share, hid)

    def share_of(array, owner):
        return lax.dynamic_index_in_dim(array, owner, 1, keepdims=False)

    gate_sum = share_of(gate_part, me)
    up_sum = share_of(up_part, me)
    for s in range(1, ways):
        owner = (me + s) % ways
        pair = jnp.stack([share_of(gate_part, owner), share_of(up_part, owner)]).astype(jnp.bfloat16)
        pair = lax.ppermute(pair, "dp", ring(ways, s))
        gate_sum = gate_sum + pair[0].astype(jnp.float32)
        up_sum = up_sum + pair[1].astype(jnp.float32)
    hidden_own = (jax.nn.silu(gate_sum) * up_sum).astype(jnp.bfloat16)
    hidden = jnp.zeros((expert_local, ways, share, hid), jnp.bfloat16)
    hidden = lax.dynamic_update_index_in_dim(hidden, hidden_own, me, 1)
    for s in range(1, ways):
        other = lax.ppermute(hidden_own, "dp", ring(ways, s))
        hidden = lax.dynamic_update_index_in_dim(hidden, other, (me - s) % ways, 1)
    hidden = hidden.reshape(expert_local, rows, hid)

    expert_out = jnp.einsum("erf,efd->erd", hidden, down_weight, preferred_element_type=jnp.float32)
    expert_out = expert_out.astype(jnp.bfloat16).reshape(1, expert_local, rows, width_local)
    returned = lax.all_to_all(expert_out, "expert", split_axis=2, concat_axis=0, tiled=True)
    returned = returned.reshape(experts_all * capacity, width_local)
    combine = (weight_expert[:, :, None] * placed.astype(jnp.float32)).reshape(
        tok_rows, experts_all * capacity
    )
    mixed = jnp.dot(
        combine,
        returned.astype(jnp.float32),
        precision=lax.Precision.HIGHEST,
        preferred_element_type=jnp.float32,
    )
    mixed = mixed.astype(jnp.bfloat16)

    for expert, part in order:
        for s in range(1, ways):
            arrival = arrivals[expert, part][s - 1]
            synced = lax.dynamic_update_slice(synced, arrival[None, None], (expert, (me - s) % ways, part * piece, 0))
    synced_down = synced.reshape(expert_local, ways * trained_rows, width_local)
    return (mixed, synced_down)


def solution(mesh):
    placed = (
        P("expert", "dp"),
        P("expert", None),
        P("expert", None),
        P("expert", "dp", None),
        P("expert", "dp", None),
        P("expert", None, "dp"),
        P("expert", "dp", None),
    )

    return jax.shard_map(
        local,
        mesh=mesh,
        in_specs=placed,
        out_specs=(P("expert", "dp"), P("expert", None, "dp")),
        check_vma=False,
    )
```

```python
import jax
import jax.numpy as jnp
from jax import lax
from jax.experimental import pallas as pl
from jax.experimental.pallas import tpu as pltpu
from jax.sharding import PartitionSpec as P


CAP = 4
PIECES = 2


def ring(size, shift):
    return [(i, (i + shift) % size) for i in range(size)]


def narrow(where, trained, synced, expert, part, piece, ways, width):
    experts, trained_rows, _ = trained.shape
    step = 96 if piece % 96 == 0 else piece
    steps = piece // step

    def body(where_ref, *refs):
        sent_ref, own_ref = refs[-2:]
        own_ref[0, 0] = refs[0][0].astype(jnp.bfloat16)
        for s in range(1, ways):
            sent_ref[s - 1] = refs[s][0].astype(jnp.bfloat16)

    def columns(s):
        return pl.BlockSpec(
            (1, step, width), lambda i, w: (expert, part * steps + i, lax.rem(w[0] + s, ways))
        )

    in_specs = [columns(s) for s in range(ways)]
    operands = [where] + [trained] * ways
    if synced is not None:
        in_specs.append(pl.BlockSpec(memory_space=pl.ANY))
        operands.append(synced)
    return pl.pallas_call(
        body,
        grid_spec=pltpu.PrefetchScalarGridSpec(
            num_scalar_prefetch=1,
            grid=(steps,),
            in_specs=in_specs,
            out_specs=[
                pl.BlockSpec((ways - 1, step, width), lambda i, w: (0, i, 0)),
                pl.BlockSpec((1, 1, step, width), lambda i, w: (expert, w[0], part * steps + i, 0)),
            ],
        ),
        out_shape=[
            jax.ShapeDtypeStruct((ways - 1, piece, width), jnp.bfloat16),
            jax.ShapeDtypeStruct((experts, ways, trained_rows, width), jnp.bfloat16),
        ],
        input_output_aliases={} if synced is None else {ways + 1: 1},
    )(*operands)


def local(tokens, routes, route_weight, gate_weight, up_weight, down_weight, trained_down):
    tok_rows, width_local = tokens.shape
    expert_local, hid, _ = down_weight.shape
    trained_rows = trained_down.shape[1]
    groups = lax.axis_size("expert")
    ways = lax.axis_size("dp")
    me = lax.axis_index("dp")
    experts_all = expert_local * groups
    capacity = CAP
    rows = groups * capacity
    share = rows // ways
    pieces = PIECES if trained_rows % (16 * PIECES) == 0 else 1
    piece = trained_rows // pieces
    where = me.astype(jnp.int32).reshape(1)

    arrivals = {}
    synced = None
    order = [(e, p) for e in range(expert_local) for p in range(pieces)]
    for expert, part in order:
        sent, synced = narrow(where, trained_down, synced, expert, part, piece, ways, width_local)
        arrivals[expert, part] = [
            lax.ppermute(sent[s - 1], "dp", ring(ways, s)) for s in range(1, ways)
        ]

    labels = lax.broadcasted_iota(jnp.int32, (1, 1, experts_all), 2)
    chosen = routes[:, :, None] == labels
    counts = jnp.sum(chosen.astype(jnp.int32), axis=1)
    earlier = jnp.cumsum(counts, axis=0) - counts
    weight_expert = jnp.sum(jnp.where(chosen, route_weight[:, :, None], 0.0), axis=1)
    slot_ids = lax.broadcasted_iota(jnp.int32, (1, 1, capacity), 2)
    placed = (counts[:, :, None] == 1) & (earlier[:, :, None] == slot_ids)
    dispatch = placed.astype(jnp.bfloat16).reshape(tok_rows, experts_all * capacity)
    outgoing = jnp.dot(dispatch.T, tokens, preferred_element_type=jnp.float32).astype(jnp.bfloat16)
    outgoing = outgoing.reshape(groups, expert_local, capacity, width_local)
    arrived = lax.all_to_all(outgoing, "expert", split_axis=0, concat_axis=2, tiled=True)
    arrived = arrived.reshape(expert_local, rows, width_local)

    gate_part = jnp.einsum("erd,edf->erf", arrived, gate_weight, preferred_element_type=jnp.float32)
    up_part = jnp.einsum("erd,edf->erf", arrived, up_weight, preferred_element_type=jnp.float32)
    gate_part = gate_part.reshape(expert_local, ways, share, hid)
    up_part = up_part.reshape(expert_local, ways, share, hid)

    def share_of(array, owner):
        return lax.dynamic_index_in_dim(array, owner, 1, keepdims=False)

    gate_sum = share_of(gate_part, me)
    up_sum = share_of(up_part, me)
    for s in range(1, ways):
        owner = (me + s) % ways
        pair = jnp.stack([share_of(gate_part, owner), share_of(up_part, owner)]).astype(jnp.bfloat16)
        pair = lax.ppermute(pair, "dp", ring(ways, s))
        gate_sum = gate_sum + pair[0].astype(jnp.float32)
        up_sum = up_sum + pair[1].astype(jnp.float32)
    hidden_own = (jax.nn.silu(gate_sum) * up_sum).astype(jnp.bfloat16)
    synced, hidden_own = lax.optimization_barrier((synced, hidden_own))
    hidden = jnp.zeros((expert_local, ways, share, hid), jnp.bfloat16)
    hidden = lax.dynamic_update_index_in_dim(hidden, hidden_own, me, 1)
    for s in range(1, ways):
        other = lax.ppermute(hidden_own, "dp", ring(ways, s))
        hidden = lax.dynamic_update_index_in_dim(hidden, other, (me - s) % ways, 1)
    hidden = hidden.reshape(expert_local, rows, hid)

    expert_out = jnp.einsum("erf,efd->erd", hidden, down_weight, preferred_element_type=jnp.float32)
    expert_out = expert_out.astype(jnp.bfloat16).reshape(1, expert_local, rows, width_local)
    returned = lax.all_to_all(expert_out, "expert", split_axis=2, concat_axis=0, tiled=True)
    returned = returned.reshape(experts_all * capacity, width_local)
    combine = (weight_expert[:, :, None] * placed.astype(jnp.float32)).reshape(
        tok_rows, experts_all * capacity
    )
    mixed = jnp.dot(
        combine,
        returned.astype(jnp.float32),
        precision=lax.Precision.HIGHEST,
        preferred_element_type=jnp.float32,
    )
    mixed = mixed.astype(jnp.bfloat16)

    for expert, part in order:
        for s in range(1, ways):
            arrival = arrivals[expert, part][s - 1]
            synced = lax.dynamic_update_slice(synced, arrival[None, None], (expert, (me - s) % ways, part * piece, 0))
    synced_down = synced.reshape(expert_local, ways * trained_rows, width_local)
    return (mixed, synced_down)


def solution(mesh):
    placed = (
        P("expert", "dp"),
        P("expert", None),
        P("expert", None),
        P("expert", "dp", None),
        P("expert", "dp", None),
        P("expert", None, "dp"),
        P("expert", "dp", None),
    )

    return jax.shard_map(
        local,
        mesh=mesh,
        in_specs=placed,
        out_specs=(P("expert", "dp"), P("expert", None, "dp")),
        check_vma=False,
    )
```
